256 devices in a mesh: wide: 16 (over x_hi, z), grp: 16 (over y, x_lo, core).
Axes of the slice: x: 4 (x_hi: 2, x_lo: 2; x = x_hi * 2 + x_lo), y: 4, z: 8, core: 2. Of those that a mesh axis runs over, the one named last changes fastest.
Arguments:
- rows_in: bfloat16 [8192, 7168], P('wide', 'grp'), may hold values from -6 to 6
- upstream: bfloat16 [8192, 7168], P('wide', 'grp'), may hold values from -1.5 to 1.5
- probs: float32 [8192], P('wide'), may hold values from 0.05 to 1
- route: int32 [8192, 1], P('wide'), may hold values from 0 to 15; in each aligned block of 512 rows (0 to 511, 512 to 1023, ...) at most 48 rows name the same one
- live: int32 [16], P('wide'), may hold values from 96 to 512, as said below
- gate_up: bfloat16 [16, 7168, 2048], P('wide', 'grp'), may hold values from -0.0625 to 0.0625
- down: bfloat16 [16, 1024, 7168], P('wide', None, 'grp'), may hold values from -0.1875 to 0.1875
Outputs:
- grad_rows: bfloat16 [8192, 7168], P('wide', 'grp')
- grad_prob: bfloat16 [8192], P('wide')
- grad_gate_up: bfloat16 [16, 7168, 2048], P('wide', 'grp')
- grad_down: bfloat16 [16, 1024, 7168], P('wide', None, 'grp')
The draws below stay inside these ranges and needn't reach their ends.
Inputs may be any that keep to these rules, and one draw needn't show every extreme that they name: `route`: in each aligned block of 512 rows no expert is named by more than 48 rows, a bound that some block reaches; every expert is named somewhere. Some block is live in full.
All inputs are finite; a program needn't handle non-finite values.
Results may differ from the reference program's by a relative error of at most 0.01.
Values may be sent and summed in bfloat16 or wider, within the bound.
A program may use at most 128 MiB of HBM per device.

```python
import math
import jax
import jax.numpy as jnp
import numpy as np
from jax import lax

D = 7168
HIDDEN_SIZE = 1024
ROWS_DEV = 512
EXPERTS = 16
CAP = 48
ROWS = 8192
N_WIDE = 16


def draw_live(key, part):
    rising = ROWS_DEV // 4 + 3 * ROWS_DEV // 4 * jnp.arange(N_WIDE, dtype=jnp.int32) // max(N_WIDE - 1, 1)
    jitter = jax.random.randint(key, (N_WIDE,), 0, ROWS_DEV // 16 + 1)
    jitter = jnp.where(jnp.arange(N_WIDE) == N_WIDE - 1, 0, jitter)
    return (rising - jitter).astype(jnp.int32)


def block_levels(stream_key, shape, pieces, low, largest):
    factor_of, own = 1.0, jax.random.fold_in(stream_key, 6)
    for dim, parts in pieces:
        draws = jnp.exp(jax.random.uniform(jax.random.fold_in(own, dim), (parts,), jnp.float32, low / len(pieces), largest / len(pieces)))
        factor_of = factor_of * jnp.repeat(draws, shape[dim] // parts).reshape([-1 if axis == dim else 1 for axis in range(len(shape))])
    return factor_of


def assign_block(own_key, own, number, rows, number_of, top, most, skew):
    ranking = jax.random.permutation(own_key, number_of)
    packed, common = shares(number_of, rows * top, most, skew, True), shares(number_of, rows * top, most, skew, False)
    places = jnp.arange(number_of)

    def named(lengths, rotation):
        used = int((lengths > 0).sum())
        fixed = max(1, used // 4)
        shifted = fixed + (places - fixed + rotation * (used - fixed)) % max(1, number_of - fixed)
        return jnp.zeros((number_of,), jnp.int32).at[ranking[jnp.where(places < fixed, places, shifted)]].set(jnp.asarray(lengths, jnp.int32))

    lengths = jnp.where(number % 4 == 0, named(packed, number // 4), named(common, number - number // 4 - 1))
    mixed = jax.random.permutation(jax.random.fold_in(own, 3), number_of)
    source_of, taker = mixed[0:number_of // 2 * 2:2], mixed[1:number_of // 2 * 2:2]
    slack = jnp.minimum(lengths[source_of] - 1, most - lengths[taker]) // 2
    slack = jnp.where((source_of == ranking[0]) | (taker == ranking[0]) | (lengths[taker] == 0), 0, jnp.maximum(slack, 0))
    shifted = jax.random.randint(jax.random.fold_in(own, 4), (number_of // 2,), 0, 1 << 20) % (slack + 1)
    lengths = lengths.at[source_of].add(-shifted).at[taker].add(shifted)
    items = jnp.searchsorted(jnp.cumsum(lengths), jnp.arange(rows * top), side="right").astype(jnp.int32)
    table = items.reshape(top, rows).T
    table = table[jax.random.permutation(jax.random.fold_in(own, 1), rows)]
    rotation = jax.random.randint(jax.random.fold_in(own, 2), (rows, 1), 0, top)
    return jnp.take_along_axis(table, (jnp.arange(top)[None, :] + rotation) % top, axis=1)


def shares(amount, total, most, skew, full):
    portions = [(1 << 20) // math.isqrt(rank ** skew) + 1 for rank in range(1, amount + 1)]
    largest = most if full else min(most, max(-(-total // amount), total * portions[0] // sum(portions)))
    least = 1 if total - largest >= amount - 1 else 0
    given, surplus = [largest] + [least] * (amount - 1), total - largest - least * (amount - 1)
    while surplus > 0:
        free = [i for i in range(1, amount) if given[i] < largest] or [i for i in range(1, amount) if given[i] < most]
        mass, remaining = sum([portions[i] for i in free]), surplus
        for i in free:
            more = min(most - given[i], max(1, remaining * portions[i] // mass), surplus)
            given[i] = given[i] + more
            surplus = surplus - more
    return np.array(given)


def noise(key, extent, deviation, limit, pieces=(), kind=jnp.bfloat16):
    drawn = jax.random.normal(key, extent, jnp.float32) * deviation
    if len(pieces) > 0:
        drawn = block_levels(key, extent, pieces, -0.22, 0.18) * drawn
    return jnp.clip(drawn, min=-limit, max=limit).astype(kind)


def setup_inputs(seed: int = 0) -> dict:
    arg_keys = jax.random.split(jax.random.key(seed), 8)
    rows_in = noise(arg_keys[0], (ROWS, D), 1.0, 6.0, ((0, 16), (1, 16)))
    upstream = noise(arg_keys[1], (ROWS, D), 0.25, 1.5, ((0, 16), (1, 16)))
    probs = jnp.clip(jnp.exp(math.log(1.0) - 2.9957323 * jax.random.uniform(arg_keys[2], (ROWS,), jnp.float32) ** block_levels(arg_keys[2], (ROWS,), ((0, 16),), -0.2, 0.2)), 0.05, 1.0)
    route_keys = jax.random.split(jax.random.fold_in(arg_keys[3], 1), ROWS // ROWS_DEV)
    route_turns = jax.random.permutation(jax.random.fold_in(arg_keys[3], 3), ROWS // ROWS_DEV)
    route = jax.vmap(lambda own, number: assign_block(jax.random.fold_in(arg_keys[3], 2), own, number, ROWS_DEV, EXPERTS, 1, CAP, 2))(route_keys, route_turns).reshape((ROWS, 1))
    live = draw_live(jax.random.fold_in(arg_keys[7], 71), 0)
    gate_up = noise(arg_keys[5], (EXPERTS, D, 2 * HIDDEN_SIZE), D ** -0.5, 0.0625, ((0, 16), (1, 16)))
    down = noise(arg_keys[6], (EXPERTS, HIDDEN_SIZE, D), HIDDEN_SIZE ** -0.5, 0.1875, ((0, 16), (2, 16)))
    return {"rows_in": rows_in, "upstream": upstream, "probs": probs, "route": route, "live": live, "gate_up": gate_up, "down": down}


BALANCE = 1.0


def activate(gate, up, grad_hidden):
    sigmoid_gate = jax.nn.sigmoid(gate)
    swish = gate * sigmoid_gate
    hidden = (swish * up).astype(jnp.bfloat16)
    grad_gate = (grad_hidden * up * sigmoid_gate * (1.0 + gate * (1.0 - sigmoid_gate))).astype(jnp.bfloat16)
    grad_up = (grad_hidden * swish).astype(jnp.bfloat16)
    return hidden, grad_gate, grad_up


def reference(rows_in, upstream, probs, route, live, gate_up, down):
    expert_of = route[:, 0].astype(jnp.int32)
    position = jnp.arange(ROWS, dtype=jnp.int32) % ROWS_DEV
    live_bound = jnp.repeat(live.astype(jnp.int32), ROWS_DEV)
    live_mask = (position < live_bound).astype(jnp.float32)
    labels = jnp.arange(EXPERTS, dtype=jnp.int32)
    onehot = (expert_of[:, None] == labels[None, :]).astype(jnp.float32)
    global_loads = jnp.sum(onehot * live_mask[:, None], axis=0)
    load_share = EXPERTS * global_loads / ROWS
    row_share = jnp.sum(onehot * load_share[None, :], axis=1)
    scaled = ((probs * live_mask)[:, None] * upstream.astype(jnp.float32)).astype(jnp.bfloat16)
    totals = jnp.sum(onehot, axis=0).astype(jnp.int32)
    starts = (jnp.cumsum(totals) - totals).astype(jnp.int32)
    row_order = jnp.argsort(expert_of, stable=True).astype(jnp.int32)
    slot_span = N_WIDE * CAP
    offsets = jnp.arange(slot_span, dtype=jnp.int32)
    hidden_width = HIDDEN_SIZE

    def one_expert(expert_index):
        filled = offsets < totals[expert_index]
        picked = row_order[jnp.minimum(starts[expert_index] + offsets, ROWS - 1)].astype(jnp.int32)
        token_rows = rows_in[picked]
        scaled_rows = jnp.where(filled[:, None], scaled[picked], jnp.zeros((), scaled.dtype))
        upward_rows = upstream[picked]
        weight_pair = gate_up[expert_index]
        weight_down = down[expert_index]
        preact = jnp.dot(token_rows, weight_pair, preferred_element_type=jnp.float32)
        grad_hidden = jnp.dot(scaled_rows, weight_down.T, preferred_element_type=jnp.float32)
        hidden, grad_gate, grad_up = activate(preact[:, :hidden_width], preact[:, hidden_width:], grad_hidden)
        grad_pair = jnp.concatenate([grad_gate, grad_up], axis=1)
        grad_local = jnp.dot(grad_pair, weight_pair.T, preferred_element_type=jnp.float32)
        outputs = jnp.dot(hidden, weight_down, preferred_element_type=jnp.float32)
        inner_sum = jnp.sum(outputs * upward_rows.astype(jnp.float32), axis=1)
        pair_grad = jnp.dot(token_rows.T, grad_pair, preferred_element_type=jnp.float32).astype(jnp.bfloat16)
        down_grad = jnp.dot(hidden.T, scaled_rows, preferred_element_type=jnp.float32).astype(jnp.bfloat16)
        grad_local = jnp.where(filled[:, None], grad_local, jnp.zeros((), grad_local.dtype))
        inner_sum = jnp.where(filled, inner_sum, jnp.zeros((), inner_sum.dtype))
        return picked, grad_local, inner_sum, pair_grad, down_grad

    picked, grad_local, inner_sum, pair_grad, down_grad = lax.map(one_expert, labels)
    flat_rows = picked.reshape(-1)
    grad_rows = jnp.zeros((ROWS, D), jnp.float32).at[flat_rows].add(grad_local.reshape(-1, D))
    inner_rows = jnp.zeros((ROWS,), jnp.float32).at[flat_rows].add(inner_sum.reshape(-1))
    inner_rows = inner_rows.astype(jnp.bfloat16).astype(jnp.float32)
    grad_prob = (live_mask * (inner_rows + BALANCE * row_share)).astype(jnp.bfloat16)
    return grad_rows.astype(jnp.bfloat16), grad_prob, pair_grad, down_grad
```

```python
import functools

import jax
import jax.numpy as jnp
from jax import lax
from jax.experimental import pallas as pl
from jax.experimental.pallas import tpu as pltpu
from jax.sharding import PartitionSpec as P

F32 = jnp.float32
BF16 = jnp.bfloat16
MESH = pl.DeviceIdType.MESH
BALANCE = 1.0
CHUNKS = 3
LANES = 128


def product(left, right, left_dim, right_dim):
    return lax.dot_general(
        left, right, (((left_dim,), (right_dim,)), ((), ())), preferred_element_type=F32
    )


def await_bytes(ref, sem):
    pltpu.make_async_copy(ref, ref, sem).wait()


def kernel(
    experts,
    live_ref,
    rows_ref,
    upstream_ref,
    probs_ref,
    route_ref,
    pair_hbm,
    down_hbm,
    grad_rows_ref,
    grad_prob_ref,
    grad_pair_ref,
    grad_down_ref,
    padded_rows,
    padded_up,
    select,
    outgoing,
    incoming,
    w_pair,
    w_down_raw,
    w_down,
    own_sum,
    core_out,
    core_in,
    y_out,
    y_in,
    x_own,
    x_out,
    x_in,
    joined,
    ret_out,
    ret_in,
    rows_acc,
    pair_acc,
    down_acc,
    count_out,
    count_in,
    w_sem,
    count_s,
    count_r,
    disp_s,
    disp_r,
    core_s,
    core_r,
    y_s,
    y_r,
    x_s,
    x_r,
    gx_s,
    gx_r,
    gy_s,
    gy_r,
    gc_s,
    gc_r,
    ret_s,
    ret_r,
):
    rows, width = rows_ref.shape
    chunks, _, slots, packed = outgoing.shape
    hidden = down_hbm.shape[0]
    padded = padded_rows.shape[1]
    spare = padded - width
    both = experts // 2
    chunk_rows = experts * slots
    half_rows = both * slots

    w = lax.axis_index("wide")
    g = lax.axis_index("grp")
    core = lax.rem(g, 2)
    place = lax.div(g, 2)
    xl = lax.rem(place, 2)
    y = lax.div(place, 2)
    other_core = g + 1 - 2 * core
    other_x = g + 2 - 4 * xl
    ys = [lax.rem(y + k, 4) for k in range(4)]

    z = lax.rem(w, 8)
    xh = lax.div(w, 8)
    wides = []
    for dx, dz in [(0, 4), (1, 4), (0, 3), (0, 5), (1, 3), (1, 5), (0, 2), (0, 6), (1, 2), (1, 6),
                   (0, 1), (0, 7), (1, 1), (1, 7), (1, 0)]:
        wides.append(lax.rem(xh + dx, 2) * 8 + lax.rem(z + dz, 8))

    barrier = pltpu.get_barrier_semaphore()

    def greet(to_w, to_g):
        pl.semaphore_signal(barrier, inc=1, device_id=(to_w, to_g), device_id_type=MESH)

    for to in wides:
        greet(to, g)
    greet(w, other_core)
    greet(w, other_x)
    for k in (1, 2, 3):
        greet(w, ys[k] * 4 + xl * 2 + core)

    pair_copy = pltpu.make_async_copy(pair_hbm, w_pair.at[pl.ds(0, width)], w_sem.at[0])
    pair_copy.start()
    down_copy = pltpu.make_async_copy(down_hbm, w_down_raw, w_sem.at[1])
    down_copy.start()

    expert_row = route_ref[...]
    position = lax.broadcasted_iota(jnp.int32, (1, rows), 1)
    inside = position < live_ref[0]
    labels = lax.broadcasted_iota(jnp.int32, (experts, rows), 0)
    onehot = jnp.where((labels == expert_row) & inside, 1.0, 0.0).astype(F32)
    earlier = jnp.where(
        lax.broadcasted_iota(jnp.int32, (rows, rows), 0)
        < lax.broadcasted_iota(jnp.int32, (rows, rows), 1),
        1.0,
        0.0,
    ).astype(BF16)
    before = product(onehot.astype(BF16), earlier, 1, 0)
    rank = jnp.sum(before * onehot, axis=0, keepdims=True)
    counts = jnp.sum(onehot, axis=1, keepdims=True)
    count_out[...] = jnp.broadcast_to(counts, count_out.shape)
    expert_f = expert_row.astype(F32)
    probs_row = probs_ref[...]

    padded_rows[:, pl.ds(0, width)] = rows_ref[...]
    padded_rows[:, pl.ds(width, spare)] = jnp.zeros((rows, spare), BF16)
    padded_up[:, pl.ds(0, width)] = upstream_ref[...]
    padded_up[:, pl.ds(width, spare)] = jnp.zeros((rows, spare), BF16)
    shift_rows = 128

    @pl.loop(0, rows // shift_rows)
    def _(i):
        at = pl.ds(pl.multiple_of(i * shift_rows, shift_rows), shift_rows)
        padded_up[at, :] = pltpu.roll(padded_up[at, :].astype(F32), spare, 1).astype(BF16)

    def remote(src, dst, send, recv, to_w, to_g):
        return pltpu.make_async_remote_copy(
            src_ref=src, dst_ref=dst, send_sem=send, recv_sem=recv,
            device_id=(to_w, to_g), device_id_type=MESH,
        )

    edge = packed - padded
    for c in range(chunks):
        offset = rank - float(c * slots)
        fits = inside & (offset >= 0.0) & (offset < float(slots))
        target = jnp.where(fits, expert_f * float(slots) + offset, -1.0)
        index = lax.broadcasted_iota(jnp.int32, (chunk_rows, rows), 0).astype(F32)
        chosen = jnp.where(index == target, 1.0, 0.0).astype(F32)
        slot_prob = jnp.sum(chosen * probs_row, axis=1, keepdims=True)
        chosen = chosen.astype(BF16)
        select[c] = chosen
        row_part = product(chosen, padded_rows[...], 1, 0).astype(BF16)
        up_part = (slot_prob * product(chosen, padded_up[...], 1, 0)).astype(BF16)
        outgoing[c, :, :, pl.ds(0, edge)] = row_part[:, :edge].reshape(experts, slots, edge)
        outgoing[c, :, :, pl.ds(edge, padded - edge)] = (
            row_part[:, edge:] + up_part[:, : padded - edge]
        ).reshape(experts, slots, padded - edge)
        outgoing[c, :, :, pl.ds(padded, packed - padded)] = up_part[:, padded - edge :].reshape(
            experts, slots, packed - padded
        )
        incoming[c, lax.rem(w, 2), lax.div(w, 2)] = outgoing[c, w]
        if c == 0:
            pl.semaphore_wait(barrier, len(wides) + 5)
        for to in wides:
            remote(
                outgoing.at[c, to],
                incoming.at[c, lax.rem(w, 2), lax.div(w, 2)],
                disp_s.at[c], disp_r.at[c], to, g,
            ).start()
    count_in[w] = count_out[...]
    for to in wides:
        remote(count_out, count_in.at[w], count_s, count_r, to, g).start()

    pair_copy.wait()
    w_pair[pl.ds(width, spare), :] = jnp.zeros((spare, w_pair.shape[1]), BF16)
    down_copy.wait()
    w_down[:, pl.ds(0, width)] = w_down_raw[...]
    w_down[:, pl.ds(width, spare)] = jnp.zeros((hidden, spare), BF16)

    @pl.loop(0, hidden // shift_rows)
    def _(i):
        at = pl.ds(pl.multiple_of(i * shift_rows, shift_rows), shift_rows)
        w_down[at, :] = pltpu.roll(w_down[at, :].astype(F32), spare, 1).astype(BF16)

    tile = 512

    def contract(c):
        await_bytes(outgoing.at[c, pl.ds(0, len(wides))], disp_r.at[c])

        def partial(part, keep):
            left = incoming[c, part, :, :, pl.ds(0, padded)].reshape(half_rows, padded)
            right = incoming[c, part, :, :, pl.ds(edge, padded)].reshape(half_rows, padded)

            @pl.loop(0, 2 * hidden // tile)
            def _(n):
                at = pl.ds(pl.multiple_of(n * tile, tile), tile)
                keep(at, product(left, w_pair[:, at], 1, 0).reshape(both, slots, tile))

            @pl.loop(0, hidden // tile)
            def _(n):
                at = pl.ds(pl.multiple_of(n * tile, tile), tile)
                to = pl.ds(pl.multiple_of(2 * hidden + n * tile, tile), tile)
                keep(to, product(right, w_down[at, :], 1, 1).reshape(both, slots, tile))

        def keep_out(at, value):
            core_out[c, :, :, at] = value.astype(BF16)

        partial(1 - core, keep_out)
        remote(core_out.at[c], core_in.at[c], core_s.at[c], core_r.at[c], w, other_core).start()

        def keep_own(at, value):
            own_sum[c, :, :, at] = value

        partial(core, keep_own)

    def reduce_y(c):
        await_bytes(core_in.at[c], core_r.at[c])
        for k in (2, 1, 3):
            at = pl.ds(2 * ys[k], 2)
            y_out[c, k - 1] = (own_sum[c, at] + core_in[c, at].astype(F32)).astype(BF16)
            remote(
                y_out.at[c, k - 1], y_in.at[c, k - 1], y_s.at[c], y_r.at[c],
                w, ys[k] * 4 + xl * 2 + core,
            ).start()

    def reduce_x(c):
        await_bytes(y_in.at[c], y_r.at[c])

        def total(part):
            at = 2 * y + part
            value = own_sum[c, at] + core_in[c, at].astype(F32)
            for k in range(3):
                value = value + y_in[c, k, part].astype(F32)
            return value

        x_out[c] = total(1 - xl).astype(BF16)
        remote(x_out.at[c], x_in.at[c], x_s.at[c], x_r.at[c], w, other_x).start()
        x_own[c] = total(xl)

    def send_on(c, at):
        for k in (2, 1, 3):
            remote(
                joined.at[c, core, at], joined.at[c, core, at], gy_s.at[c], gy_r.at[c],
                w, ys[k] * 4 + xl * 2 + core,
            ).start()

    def activate(c):
        await_bytes(x_in.at[c], x_r.at[c])
        value = x_own[c] + x_in[c].astype(F32)
        gate = value[:, :hidden]
        up = value[:, hidden : 2 * hidden]
        grad_hidden = value[:, 2 * hidden :]
        sigmoid_gate = jax.nn.sigmoid(gate)
        swish = gate * sigmoid_gate
        act = (swish * up).astype(BF16)
        grad_gate = grad_hidden * up * sigmoid_gate * (1.0 + gate * (1.0 - sigmoid_gate))
        joined[c, core, place, :, pl.ds(0, hidden)] = act
        joined[c, core, place, :, pl.ds(hidden, hidden)] = grad_gate.astype(BF16)
        joined[c, core, place, :, pl.ds(2 * hidden, hidden)] = (grad_hidden * swish).astype(BF16)
        inner = jnp.sum(act.astype(F32) * grad_hidden, axis=1, keepdims=True)
        high = inner.astype(BF16).astype(F32)
        lane = lax.broadcasted_iota(jnp.int32, (slots, LANES), 1)
        at = width - (padded - LANES)
        split = jnp.where(lane == at, high, jnp.where(lane == at + 1, inner - high, 0.0))
        joined[c, core, place, :, pl.ds(3 * hidden, LANES)] = split.astype(BF16)
        remote(
            joined.at[c, core, place], joined.at[c, core, place], gx_s.at[c], gx_r.at[c], w, other_x
        ).start()
        send_on(c, place)

    def forward(c):
        await_bytes(joined.at[c, 0, 0], gx_r.at[c])
        send_on(c, 2 * y + 1 - xl)

    def share(c):
        await_bytes(joined.at[c, 0, pl.ds(0, 6)], gy_r.at[c])
        remote(
            joined.at[c, core], joined.at[c, core], gc_s.at[c], gc_r.at[c], w, other_core
        ).start()

    def give_back(c):
        await_bytes(joined.at[c, 0], gc_r.at[c])

        @pl.loop(0, 2)
        def _(part):
            pairs = joined[c, part, :, :, pl.ds(hidden, 2 * hidden)].reshape(half_rows, 2 * hidden)
            inner = joined[c, part, :, :, pl.ds(3 * hidden, LANES)].reshape(half_rows, LANES)
            value = product(pairs, w_pair[...], 1, 1)
            cut = padded - LANES
            ret_out[c, part, :, :, pl.ds(0, cut)] = (
                value[:, :cut].astype(BF16).reshape(both, slots, cut)
            )
            ret_out[c, part, :, :, pl.ds(cut, LANES)] = (
                value[:, cut:].astype(BF16) + inner
            ).reshape(both, slots, LANES)

        ret_in[c, w] = ret_out[c, lax.rem(w, 2), lax.div(w, 2)]
        for to in wides:
            remote(
                ret_out.at[c, lax.rem(to, 2), lax.div(to, 2)], ret_in.at[c, w],
                ret_s.at[c], ret_r.at[c], to, g,
            ).start()

    def weigh(c):
        left = incoming[c, :, :, :, pl.ds(0, padded)].reshape(chunk_rows, padded)
        right = incoming[c, :, :, :, pl.ds(edge, padded)].reshape(chunk_rows, padded)
        step = 256

        @pl.loop(0, 2 * hidden // step)
        def _(n):
            at = pl.ds(pl.multiple_of(n * step, step), step)
            src = pl.ds(pl.multiple_of(hidden + n * step, step), step)
            value = product(left, joined[c, :, :, :, src].reshape(chunk_rows, step), 0, 0)
            if c > 0:
                value = value + pair_acc[:, at]
            if c == chunks - 1:
                grad_pair_ref[:, at] = value[:width].astype(BF16)
            else:
                pair_acc[:, at] = value

        @pl.loop(0, hidden // step)
        def _(n):
            at = pl.ds(pl.multiple_of(n * step, step), step)
            value = product(joined[c, :, :, :, at].reshape(chunk_rows, step), right, 0, 0)
            if c > 0:
                value = value + down_acc[at, :]
            if c == chunks - 1:
                grad_down_ref[at, :] = value.astype(BF16)
            else:
                down_acc[at, :] = value

    def receive(c, inner):
        await_bytes(outgoing.at[c, pl.ds(0, len(wides)), :, pl.ds(0, padded)], ret_r.at[c])
        back = ret_in[c].reshape(chunk_rows, padded)
        chosen = select[c]
        value = product(chosen, back, 0, 0)
        if c > 0:
            value = value + rows_acc[...]
        if c == chunks - 1:
            grad_rows_ref[...] = value[:, :width].astype(BF16)
        else:
            rows_acc[...] = value
        return inner + product(back[:, padded - LANES :], chosen, 0, 0)

    contract(0)
    reduce_y(0)
    contract(1)
    reduce_y(1)
    reduce_x(0)
    activate(0)
    forward(0)
    contract(2)
    reduce_y(2)
    reduce_x(1)
    activate(1)
    share(0)
    forward(1)
    give_back(0)
    weigh(0)
    reduce_x(2)
    activate(2)
    share(1)
    forward(2)
    give_back(1)
    weigh(1)
    share(2)
    give_back(2)
    weigh(2)
    inner = jnp.zeros((LANES, rows), F32)
    for c in range(chunks):
        inner = receive(c, inner)

    await_bytes(count_in.at[pl.ds(0, len(wides))], count_r)
    loads = jnp.sum(count_in[...], axis=0)[:, :1]
    share_row = jnp.sum(
        jnp.where(labels == expert_row, 1.0, 0.0) * (loads * (1.0 / rows)), axis=0, keepdims=True
    )
    at = width - (padded - LANES)
    inner_row = (inner[at : at + 1] + inner[at + 1 : at + 2]) / probs_row
    inner_row = inner_row.astype(BF16).astype(F32)
    grad_prob_ref[...] = jnp.where(inside, inner_row + BALANCE * share_row, 0.0).astype(BF16)

    await_bytes(count_in.at[pl.ds(0, len(wides))], count_s)
    for c in range(chunks):
        await_bytes(outgoing.at[c, pl.ds(0, len(wides))], disp_s.at[c])
        await_bytes(core_out.at[c], core_s.at[c])
        await_bytes(y_out.at[c], y_s.at[c])
        await_bytes(x_out.at[c], x_s.at[c])
        await_bytes(joined.at[c, 0, 0], gx_s.at[c])
        await_bytes(joined.at[c, 0, pl.ds(0, 6)], gy_s.at[c])
        await_bytes(joined.at[c, 0], gc_s.at[c])
        await_bytes(outgoing.at[c, pl.ds(0, len(wides)), :, pl.ds(0, padded)], ret_s.at[c])


def on_device(rows_in, upstream, probs, route, live, gate_up, down):
    rows, width = rows_in.shape
    experts = lax.axis_size("wide")
    hidden = down.shape[1]
    slots = rows * 3 // (2 * experts) // CHUNKS
    padded = -(-width // LANES) * LANES
    packed = 2 * width
    both = experts // 2
    total = 3 * hidden
    vmem = pltpu.VMEM
    dma = pltpu.SemaphoreType.DMA
    each = dma((CHUNKS,))
    scratch = [
        vmem((rows, padded), BF16),
        vmem((rows, padded), BF16),
        vmem((CHUNKS, experts * slots, rows), BF16),
        vmem((CHUNKS, experts, slots, packed), BF16),
        vmem((CHUNKS, 2, both, slots, packed), BF16),
        vmem((padded, 2 * hidden), BF16),
        vmem((hidden, width), BF16),
        vmem((hidden, padded), BF16),
        vmem((CHUNKS, both, slots, total), F32),
        vmem((CHUNKS, both, slots, total), BF16),
        vmem((CHUNKS, both, slots, total), BF16),
        vmem((CHUNKS, 3, 2, slots, total), BF16),
        vmem((CHUNKS, 3, 2, slots, total), BF16),
        vmem((CHUNKS, slots, total), F32),
        vmem((CHUNKS, slots, total), BF16),
        vmem((CHUNKS, slots, total), BF16),
        vmem((CHUNKS, 2, both, slots, total + LANES), BF16),
        vmem((CHUNKS, 2, both, slots, padded), BF16),
        vmem((CHUNKS, experts, slots, padded), BF16),
        vmem((rows, padded), F32),
        vmem((padded, 2 * hidden), F32),
        vmem((hidden, padded), F32),
        vmem((experts, LANES), F32),
        vmem((experts, experts, LANES), F32),
        dma((2,)),
        dma,
        dma,
    ] + [each] * 16
    in_vmem = pl.BlockSpec(memory_space=pltpu.VMEM)
    out = pl.pallas_call(
        functools.partial(kernel, experts),
        out_shape=(
            jax.ShapeDtypeStruct((rows, width), BF16),
            jax.ShapeDtypeStruct((1, rows), BF16),
            jax.ShapeDtypeStruct((width, 2 * hidden), BF16),
            jax.ShapeDtypeStruct((hidden, padded), BF16),
        ),
        in_specs=[
            pl.BlockSpec(memory_space=pltpu.SMEM),
            in_vmem,
            in_vmem,
            in_vmem,
            in_vmem,
            pl.BlockSpec(memory_space=pl.ANY),
            pl.BlockSpec(memory_space=pl.ANY),
        ],
        out_specs=(in_vmem,) * 4,
        scratch_shapes=scratch,
        compiler_params=pltpu.CompilerParams(
            collective_id=0, has_side_effects=True, vmem_limit_bytes=60 * 2**20
        ),
    )(
        live,
        rows_in,
        upstream,
        probs.reshape(1, rows),
        route.reshape(1, rows),
        gate_up[0],
        down[0],
    )
    grad_rows, grad_prob, grad_pair, grad_down = out
    return (
        grad_rows,
        grad_prob.reshape(rows),
        grad_pair[None],
        grad_down[None, :, padded - width :],
    )


def solution(mesh):
    return jax.shard_map(
        on_device,
        mesh=mesh,
        in_specs=(
            P("wide", "grp"),
            P("wide", "grp"),
            P("wide"),
            P("wide", None),
            P("wide"),
            P("wide", "grp", None),
            P("wide", None, "grp"),
        ),
        out_specs=(P("wide", "grp"), P("wide"), P("wide", "grp", None), P("wide", None, "grp")),
        check_vma=False,
    )
```

```python
import functools

import jax
import jax.numpy as jnp
from jax import lax
from jax.experimental import pallas as pl
from jax.experimental.pallas import tpu as pltpu
from jax.sharding import PartitionSpec as P

F32 = jnp.float32
BF16 = jnp.bfloat16
MESH = pl.DeviceIdType.MESH
BALANCE = 1.0
PARTS = (2, 2, 1, 1)
LANES = 128


def product(left, right, left_dim, right_dim):
    return lax.dot_general(
        left, right, (((left_dim,), (right_dim,)), ((), ())), preferred_element_type=F32
    )


def await_bytes(ref, sem, name="wait"):
    with jax.named_scope(name):
        pltpu.make_async_copy(ref, ref, sem).wait()


def kernel(
    experts,
    live_ref,
    rows_hbm,
    upstream_hbm,
    probs_ref,
    route_ref,
    pair_hbm,
    down_hbm,
    rows_vm,
    grad_prob_ref,
    pair_vm,
    down_vm,
    padded_rows,
    padded_up,
    select,
    outgoing,
    incoming,
    w_pair,
    w_down,
    own_sum,
    core_out,
    core_in,
    far_out,
    far_in,
    y_out,
    y_in,
    x_own,
    x_out,
    x_in,
    joined,
    ret_out,
    ret_in,
    rows_acc,
    count_out,
    count_in,
    w_sem,
    count_s,
    count_r,
    disp_s,
    disp_r,
    core_s,
    core_r,
    far_s,
    far_r,
    y_s,
    y_r,
    x_s,
    x_r,
    gx_s,
    gx_r,
    gy_s,
    gy_r,
    gz_s,
    gz_r,
    gf_s,
    gf_r,
    gc_s,
    gc_r,
    ret_s,
    ret_r,
):
    width, rows = rows_hbm.shape
    chunks = len(outgoing)
    packed = outgoing[0].shape[2]
    sizes = [ref.shape[1] for ref in outgoing]
    firsts = [sum(sizes[:c]) for c in range(chunks)]
    hidden = down_hbm.shape[1]
    padded = padded_rows.shape[0]
    spare = padded - width
    both = experts // 2

    w = lax.axis_index("wide")
    g = lax.axis_index("grp")
    core = lax.rem(g, 2)
    place = lax.div(g, 2)
    xl = lax.rem(place, 2)
    y = lax.div(place, 2)
    other_core = g + 1 - 2 * core
    other_x = g + 2 - 4 * xl
    ys = [lax.rem(y + k, 4) for k in range(4)]

    z = lax.rem(w, 8)
    xh = lax.div(w, 8)
    wides = []
    for dx, dz in [(0, 4), (1, 4), (0, 3), (0, 5), (1, 3), (1, 5), (0, 2), (0, 6), (1, 2), (1, 6),
                   (0, 1), (0, 7), (1, 1), (1, 7), (1, 0)]:
        wides.append(lax.rem(xh + dx, 2) * 8 + lax.rem(z + dz, 8))

    barrier = pltpu.get_barrier_semaphore()

    def greet(to_w, to_g):
        pl.semaphore_signal(barrier, inc=1, device_id=(to_w, to_g), device_id_type=MESH)

    for to in wides:
        greet(to, g)
    greet(w, other_core)
    greet(w, other_x)
    for k in (1, 3):
        greet(w, ys[k] * 4 + xl * 2 + core)

    into = (
        padded_rows.at[pl.ds(0, width)],
        padded_up.at[pl.ds(spare, width)],
        w_pair.at[pl.ds(0, width)],
        w_down.at[pl.ds(spare, width)],
    )
    copies = [
        pltpu.make_async_copy(src, dst, w_sem.at[i])
        for i, (src, dst) in enumerate(zip((rows_hbm, upstream_hbm, pair_hbm, down_hbm), into))
    ]
    for copy in copies:
        copy.start()
    padded_rows[pl.ds(width, spare), :] = jnp.zeros((spare, rows), BF16)
    padded_up[pl.ds(0, spare), :] = jnp.zeros((spare, rows), BF16)
    w_pair[pl.ds(width, spare), :] = jnp.zeros((spare, w_pair.shape[1]), BF16)
    w_down[pl.ds(0, spare), :] = jnp.zeros((spare, hidden), BF16)

    expert_row = route_ref[...]
    position = lax.broadcasted_iota(jnp.int32, (1, rows), 1)
    inside = position < live_ref[0]
    labels = lax.broadcasted_iota(jnp.int32, (experts, rows), 0)
    onehot = jnp.where((labels == expert_row) & inside, 1.0, 0.0).astype(F32)
    earlier = jnp.where(
        lax.broadcasted_iota(jnp.int32, (rows, rows), 0)
        < lax.broadcasted_iota(jnp.int32, (rows, rows), 1),
        1.0,
        0.0,
    ).astype(BF16)
    before = product(onehot.astype(BF16), earlier, 1, 0)
    rank = jnp.sum(before * onehot, axis=0, keepdims=True)
    counts = jnp.sum(onehot, axis=1, keepdims=True)
    count_out[...] = jnp.broadcast_to(counts, count_out.shape)
    expert_f = expert_row.astype(F32)
    probs_row = probs_ref[...]

    with jax.named_scope("load"):
        copies[0].wait()
        copies[1].wait()

    def remote(src, dst, send, recv, to_w, to_g):
        return pltpu.make_async_remote_copy(
            src_ref=src, dst_ref=dst, send_sem=send, recv_sem=recv,
            device_id=(to_w, to_g), device_id_type=MESH,
        )

    edge = packed - padded
    for c in range(chunks):
        slots = sizes[c]
        chunk_rows = experts * slots
        with jax.named_scope(f"arrange{c}"):
            offset = rank - float(firsts[c])
            fits = inside & (offset >= 0.0) & (offset < float(slots))
            target = jnp.where(fits, expert_f * float(slots) + offset, -1.0)
            index = lax.broadcasted_iota(jnp.int32, (chunk_rows, rows), 0).astype(F32)
            chosen = jnp.where(index == target, 1.0, 0.0).astype(F32)
            slot_prob = jnp.sum(chosen * probs_row, axis=1, keepdims=True)
            chosen = chosen.astype(BF16)
            select[c][...] = chosen
            row_part = product(chosen, padded_rows[...], 1, 1).astype(BF16)
            up_part = (slot_prob * product(chosen, padded_up[...], 1, 1)).astype(BF16)
            outgoing[c][:, :, pl.ds(0, edge)] = row_part[:, :edge].reshape(experts, slots, edge)
            outgoing[c][:, :, pl.ds(edge, padded - edge)] = (
                row_part[:, edge:] + up_part[:, : padded - edge]
            ).reshape(experts, slots, padded - edge)
            outgoing[c][:, :, pl.ds(padded, packed - padded)] = up_part[:, padded - edge :].reshape(
                experts, slots, packed - padded
            )
            incoming[c][lax.rem(w, 2), lax.div(w, 2)] = outgoing[c][w]
        if c == 0:
            with jax.named_scope("barrier"):
                pl.semaphore_wait(barrier, len(wides) + 4)
        with jax.named_scope(f"send{c}"):
            for to in wides:
                remote(
                    outgoing[c].at[to],
                    incoming[c].at[lax.rem(w, 2), lax.div(w, 2)],
                    disp_s.at[c], disp_r.at[c], to, g,
                ).start()
    count_in[w] = count_out[...]
    for to in wides:
        remote(count_out, count_in.at[w], count_s, count_r, to, g).start()

    with jax.named_scope("load2"):
        copies[2].wait()
        copies[3].wait()

    tile = 512

    def contract(c):
        slots = sizes[c]
        half_rows = both * slots
        await_bytes(outgoing[c].at[pl.ds(0, len(wides))], disp_r.at[c])

        def partial(parts, keep):
            def operand(first):
                blocks = [incoming[c][part, :, :, pl.ds(first, padded)] for part in parts]
                return jnp.concatenate(
                    [block.reshape(half_rows, padded) for block in blocks], axis=0
                )

            left, right = operand(0), operand(edge)

            @pl.loop(0, 2 * hidden // tile)
            def _(n):
                at = pl.ds(pl.multiple_of(n * tile, tile), tile)
                keep(at, product(left, w_pair[:, at], 1, 0))

            @pl.loop(0, hidden // tile)
            def _(n):
                at = pl.ds(pl.multiple_of(n * tile, tile), tile)
                to = pl.ds(pl.multiple_of(2 * hidden + n * tile, tile), tile)
                keep(to, product(right, w_down[:, at], 1, 0))

        def keep_out(at, value):
            core_out[c][:, :, at] = value[:half_rows].reshape(both, slots, tile).astype(BF16)

        def keep_own(at, value):
            own_sum[c][:, :, at] = value[-half_rows:].reshape(both, slots, tile)

        def keep_both(at, value):
            keep_out(at, value)
            keep_own(at, value)

        def exchange():
            remote(core_out[c], core_in[c], core_s.at[c], core_r.at[c], w, other_core).start()

        if half_rows < LANES:
            partial((1 - core, core), keep_both)
            exchange()
        else:
            partial((1 - core,), keep_out)
            exchange()
            partial((core,), keep_own)

    def to_y(k, src, dst, send, recv):
        remote(src, dst, send, recv, w, ys[k] * 4 + xl * 2 + core).start()

    def partial_sum(c, k, part):
        at = 2 * ys[k] + part
        return own_sum[c][at] + core_in[c][at].astype(F32)

    def reduce_y(c):
        await_bytes(core_in[c], core_r.at[c])
        for side in (0, 1):
            far_out[c][side] = partial_sum(c, 2, side).astype(BF16)
            to_y((1, 3)[side], far_out[c].at[side], far_in[c].at[side], far_s.at[c], far_r.at[c])
        for side in (0, 1):
            y_out[c][side, 1 - side] = partial_sum(c, (1, 3)[side], 1 - side).astype(BF16)
            to_y(
                (1, 3)[side], y_out[c].at[side, 1 - side], y_in[c].at[side, 1 - side],
                y_s.at[c], y_r.at[c],
            )

    def relay_y(c):
        await_bytes(far_in[c], far_r.at[c])
        for side in (0, 1):
            value = partial_sum(c, (1, 3)[side], side) + far_in[c][side].astype(F32)
            y_out[c][side, side] = value.astype(BF16)
            to_y(
                (1, 3)[side], y_out[c].at[side, side], y_in[c].at[side, side], y_s.at[c], y_r.at[c]
            )

    def reduce_x(c):
        await_bytes(y_in[c], y_r.at[c])

        def total(part):
            value = partial_sum(c, 0, part)
            for side in (0, 1):
                value = value + y_in[c][side, part].astype(F32)
            return value

        x_out[c][...] = total(1 - xl).astype(BF16)
        remote(x_out[c], x_in[c], x_s.at[c], x_r.at[c], w, other_x).start()
        x_own[c][...] = total(xl)

    def activate(c):
        slots = sizes[c]
        await_bytes(x_in[c], x_r.at[c])
        value = x_own[c][...] + x_in[c][...].astype(F32)
        gate = value[:, :hidden]
        up = value[:, hidden : 2 * hidden]
        grad_hidden = value[:, 2 * hidden :]
        sigmoid_gate = jax.nn.sigmoid(gate)
        swish = gate * sigmoid_gate
        act = (swish * up).astype(BF16)
        grad_gate = grad_hidden * up * sigmoid_gate * (1.0 + gate * (1.0 - sigmoid_gate))
        joined[c][core, place, :, pl.ds(0, hidden)] = act
        joined[c][core, place, :, pl.ds(hidden, hidden)] = grad_gate.astype(BF16)
        joined[c][core, place, :, pl.ds(2 * hidden, hidden)] = (grad_hidden * swish).astype(BF16)
        inner = jnp.sum(act.astype(F32) * grad_hidden, axis=1, keepdims=True)
        high = inner.astype(BF16).astype(F32)
        lane = lax.broadcasted_iota(jnp.int32, (slots, LANES), 1)
        at = width - (padded - LANES)
        split = jnp.where(lane == at, high, jnp.where(lane == at + 1, inner - high, 0.0))
        joined[c][core, place, :, pl.ds(3 * hidden, LANES)] = split.astype(BF16)
        for k in (1, 3):
            piece_to_y(c, k, place, gy_s, gy_r)
        remote(
            joined[c].at[core, place], joined[c].at[core, place], gx_s.at[c], gx_r.at[c], w, other_x
        ).start()

    def piece_to_y(c, k, at, send, recv):
        piece = joined[c].at[core, at]
        to_y(k, piece, piece, send.at[c], recv.at[c])

    def forward(c):
        await_bytes(joined[c].at[0, 0], gx_r.at[c])
        for k in (1, 3):
            piece_to_y(c, k, 2 * y + 1 - xl, gz_s, gz_r)

    def pass_near(c):
        await_bytes(joined[c].at[0, pl.ds(0, 2)], gy_r.at[c])
        piece_to_y(c, 1, 2 * ys[3] + xl, gf_s, gf_r)

    def pass_far(c):
        await_bytes(joined[c].at[0, pl.ds(0, 2)], gz_r.at[c])
        piece_to_y(c, 3, 2 * ys[1] + 1 - xl, gf_s, gf_r)
        for k in (0, 1, 3):
            share(c, k)

    def share(c, k):
        pieces = joined[c].at[core, pl.ds(2 * ys[k], 2)]
        remote(pieces, pieces, gc_s.at[c], gc_r.at[c], w, other_core).start()

    def share_last(c):
        await_bytes(joined[c].at[0, pl.ds(0, 2)], gf_r.at[c])
        share(c, 2)

    def give_back(c):
        slots = sizes[c]
        half_rows = both * slots
        await_bytes(joined[c].at[0], gc_r.at[c])
        cut = padded - LANES
        for part in (0, 1):
            pairs = joined[c][part, :, :, pl.ds(hidden, 2 * hidden)].reshape(half_rows, 2 * hidden)
            inner = joined[c][part, :, :, pl.ds(3 * hidden, LANES)].reshape(half_rows, LANES)
            value = product(pairs, w_pair[...], 1, 1)
            ret_out[c][part, :, :, pl.ds(0, cut)] = (
                value[:, :cut].astype(BF16).reshape(both, slots, cut)
            )
            ret_out[c][part, :, :, pl.ds(cut, LANES)] = (
                value[:, cut:].astype(BF16) + inner
            ).reshape(both, slots, LANES)
        ret_in[c][w] = ret_out[c][lax.rem(w, 2), lax.div(w, 2)]
        for to in wides:
            remote(
                ret_out[c].at[lax.rem(to, 2), lax.div(to, 2)], ret_in[c].at[w],
                ret_s.at[c], ret_r.at[c], to, g,
            ).start()

    def weigh():
        step = 256
        lefts, rights = [], []
        for c in range(chunks):
            chunk_rows = experts * sizes[c]
            lefts.append(incoming[c][:, :, :, pl.ds(0, padded)].reshape(chunk_rows, padded).T)
            rights.append(incoming[c][:, :, :, pl.ds(edge, padded)].reshape(chunk_rows, padded).T)

        def total(parts, at):
            value = 0.0
            for c in range(chunks):
                right = joined[c][:, :, :, at].reshape(experts * sizes[c], step)
                value = value + product(parts[c], right, 1, 0)
            return value

        @pl.loop(0, 2 * hidden // step)
        def _(n):
            at = pl.ds(pl.multiple_of(n * step, step), step)
            src = pl.ds(pl.multiple_of(hidden + n * step, step), step)
            pair_vm[:, at] = total(lefts, src)[:width].astype(BF16)

        @pl.loop(0, hidden // step)
        def _(n):
            at = pl.ds(pl.multiple_of(n * step, step), step)
            down_vm[:, at] = total(rights, at)[spare:].astype(BF16)

    def receive(c):
        chunk_rows = experts * sizes[c]
        await_bytes(outgoing[c].at[pl.ds(0, len(wides)), :, pl.ds(0, padded)], ret_r.at[c])
        value = product(ret_in[c][...].reshape(chunk_rows, padded), select[c][...], 0, 0)
        rows_acc[...] = value if c == 0 else rows_acc[...] + value

    order = (
        (contract, 0), (reduce_y, 0), (relay_y, 0), (reduce_x, 0), (contract, 1), (reduce_y, 1),
        (activate, 0), (relay_y, 1), (contract, 2), (reduce_y, 2), (forward, 0), (pass_near, 0),
        (contract, 3), (reduce_y, 3), (reduce_x, 1), (relay_y, 2), (pass_far, 0), (activate, 1),
        (relay_y, 3), (share_last, 0), (forward, 1), (reduce_x, 2), (give_back, 0), (activate, 2),
        (pass_near, 1), (pass_far, 1), (reduce_x, 3), (activate, 3), (forward, 2),
        (share_last, 1), (forward, 3), (give_back, 1), (pass_near, 2), (pass_near, 3),
        (pass_far, 2), (pass_far, 3), (share_last, 2), (share_last, 3), (give_back, 2),
        (give_back, 3),
    )
    for stage, c in order:
        with jax.named_scope(stage.__name__ + str(c)):
            stage(c)
    with jax.named_scope("weigh"):
        weigh()
    for c in range(chunks):
        with jax.named_scope(f"receive{c}"):
            receive(c)
    rows_vm[...] = rows_acc[pl.ds(0, width), :].astype(BF16)

    await_bytes(count_in.at[pl.ds(0, len(wides))], count_r)
    loads = jnp.sum(count_in[...], axis=0)[:, :1]
    share_row = jnp.sum(
        jnp.where(labels == expert_row, 1.0, 0.0) * (loads * (1.0 / rows)), axis=0, keepdims=True
    )
    inner = rows_acc[pl.ds(width, 8), :]
    inner_row = (inner[0:1] + inner[1:2]) / probs_row
    inner_row = inner_row.astype(BF16).astype(F32)
    grad_prob_ref[...] = jnp.where(inside, inner_row + BALANCE * share_row, 0.0)

    await_bytes(count_in.at[pl.ds(0, len(wides))], count_s)
    for c in range(chunks):
        await_bytes(outgoing[c].at[pl.ds(0, len(wides))], disp_s.at[c])
        await_bytes(core_out[c], core_s.at[c])
        await_bytes(far_out[c], far_s.at[c])
        await_bytes(y_out[c], y_s.at[c])
        await_bytes(x_out[c], x_s.at[c])
        await_bytes(joined[c].at[0, 0], gx_s.at[c])
        for sem in (gy_s, gz_s, gf_s):
            await_bytes(joined[c].at[0, pl.ds(0, 2)], sem.at[c])
        await_bytes(joined[c].at[0], gc_s.at[c])
        await_bytes(outgoing[c].at[pl.ds(0, len(wides)), :, pl.ds(0, padded)], ret_s.at[c])


def store_kernel(rows_vm, prob_vm, pair_vm, down_vm, rows_hbm, prob_ref, pair_hbm, down_hbm, sem):
    copies = [
        pltpu.make_async_copy(src, dst, sem.at[i])
        for i, (src, dst) in enumerate(((pair_vm, pair_hbm), (down_vm, down_hbm), (rows_vm, rows_hbm)))
    ]
    for copy in copies:
        copy.start()
    prob_ref[...] = prob_vm[...].reshape(prob_ref.shape).astype(BF16)
    for copy in copies:
        copy.wait()


def on_device(rows_in, upstream, probs, route, live, gate_up, down):
    rows, width = rows_in.shape
    experts = lax.axis_size("wide")
    hidden = down.shape[1]
    unit = rows * 3 // (2 * experts) // sum(PARTS)
    sizes = [part * unit for part in PARTS]
    chunks = len(sizes)
    padded = -(-width // LANES) * LANES
    packed = 2 * width
    both = experts // 2
    total = 3 * hidden
    vmem = pltpu.VMEM
    dma = pltpu.SemaphoreType.DMA
    each = dma((chunks,))
    scratch = [
        vmem((padded, rows), BF16),
        vmem((padded, rows), BF16),
        [vmem((experts * slots, rows), BF16) for slots in sizes],
        [vmem((experts, slots, packed), BF16) for slots in sizes],
        [vmem((2, both, slots, packed), BF16) for slots in sizes],
        vmem((padded, 2 * hidden), BF16),
        vmem((padded, hidden), BF16),
        [vmem((both, slots, total), F32) for slots in sizes],
        [vmem((both, slots, total), BF16) for slots in sizes],
        [vmem((both, slots, total), BF16) for slots in sizes],
        [vmem((2, slots, total), BF16) for slots in sizes],
        [vmem((2, slots, total), BF16) for slots in sizes],
        [vmem((2, 2, slots, total), BF16) for slots in sizes],
        [vmem((2, 2, slots, total), BF16) for slots in sizes],
        [vmem((slots, total), F32) for slots in sizes],
        [vmem((slots, total), BF16) for slots in sizes],
        [vmem((slots, total), BF16) for slots in sizes],
        [vmem((2, both, slots, total + LANES), BF16) for slots in sizes],
        [vmem((2, both, slots, padded), BF16) for slots in sizes],
        [vmem((experts, slots, padded), BF16) for slots in sizes],
        vmem((padded, rows), F32),
        vmem((experts, LANES), F32),
        vmem((experts, experts, LANES), F32),
        dma((4,)),
        dma,
        dma,
    ] + [each] * 22
    in_vmem = pl.BlockSpec(memory_space=pltpu.VMEM)
    anywhere = pl.BlockSpec(memory_space=pltpu.HBM)
    out = pl.pallas_call(
        functools.partial(kernel, experts),
        out_shape=(
            vmem((width, rows), BF16),
            vmem((1, rows), F32),
            vmem((width, 2 * hidden), BF16),
            vmem((width, hidden), BF16),
        ),
        in_specs=[
            pl.BlockSpec(memory_space=pltpu.SMEM),
            anywhere,
            anywhere,
            in_vmem,
            in_vmem,
            anywhere,
            anywhere,
        ],
        out_specs=(in_vmem,) * 4,
        scratch_shapes=scratch,
        compiler_params=pltpu.CompilerParams(
            collective_id=0, has_side_effects=True, vmem_limit_bytes=121 * 2**19
        ),
    )(
        live,
        rows_in.T,
        upstream.T,
        probs.reshape(1, rows),
        route.reshape(1, rows),
        gate_up[0],
        down[0].T,
    )
    grad_rows, grad_prob, grad_pair, grad_down = pl.pallas_call(
        store_kernel,
        out_shape=(
            jax.ShapeDtypeStruct((width, rows), BF16),
            jax.ShapeDtypeStruct((rows,), BF16),
            jax.ShapeDtypeStruct((width, 2 * hidden), BF16),
            jax.ShapeDtypeStruct((width, hidden), BF16),
        ),
        in_specs=[in_vmem] * 4,
        out_specs=(anywhere, in_vmem, anywhere, anywhere),
        scratch_shapes=[dma((3,))],
        compiler_params=pltpu.CompilerParams(vmem_limit_bytes=2**20),
    )(*out)
    return (
        grad_rows.T,
        grad_prob,
        grad_pair[None],
        grad_down.T[None],
    )


def solution(mesh):
    return jax.shard_map(
        on_device,
        mesh=mesh,
        in_specs=(
            P("wide", "grp"),
            P("wide", "grp"),
            P("wide"),
            P("wide", None),
            P("wide"),
            P("wide", "grp", None),
            P("wide", None, "grp"),
        ),
        out_specs=(P("wide", "grp"), P("wide"), P("wide", "grp", None), P("wide", None, "grp")),
        check_vma=False,
    )
```

```python
import functools

import jax
import jax.numpy as jnp
from jax import lax
from jax.experimental import pallas as pl
from jax.experimental.pallas import tpu as pltpu
from jax.sharding import PartitionSpec as P

F32 = jnp.float32
BF16 = jnp.bfloat16
MESH = pl.DeviceIdType.MESH
BALANCE = 1.0
PARTS = (1, 2, 2, 1)
COLUMN_FIRST = ()
LANES = 128


def product(left, right, left_dim, right_dim):
    return lax.dot_general(
        left, right, (((left_dim,), (right_dim,)), ((), ())), preferred_element_type=F32
    )


def await_bytes(ref, sem, name="wait"):
    with jax.named_scope(name):
        pltpu.make_async_copy(ref, ref, sem).wait()


def kernel(
    experts,
    live_ref,
    rows_hbm,
    upstream_hbm,
    probs_ref,
    route_ref,
    pair_hbm,
    down_hbm,
    rows_vm,
    grad_prob_ref,
    pair_vm,
    down_vm,
    padded_rows,
    padded_up,
    select,
    outgoing,
    incoming,
    w_pair,
    w_down,
    own_sum,
    core_out,
    core_in,
    far_out,
    far_in,
    y_out,
    y_in,
    x_own,
    x_out,
    x_in,
    joined,
    ret_out,
    ret_in,
    rows_acc,
    count_out,
    count_in,
    w_sem,
    count_s,
    count_r,
    disp_s,
    disp_r,
    core_s,
    core_r,
    far_s,
    far_r,
    y_s,
    y_r,
    x_s,
    x_r,
    gx_s,
    gx_r,
    gy_s,
    gy_r,
    gz_s,
    gz_r,
    gf_s,
    gf_r,
    gc_s,
    gc_r,
    ret_s,
    ret_r,
):
    width, rows = rows_hbm.shape
    chunks = len(outgoing)
    packed = outgoing[0].shape[2]
    sizes = [ref.shape[1] for ref in outgoing]
    firsts = [sum(sizes[:c]) for c in range(chunks)]
    hidden = down_hbm.shape[1]
    padded = padded_rows.shape[0]
    spare = padded - width
    both = experts // 2

    w = lax.axis_index("wide")
    g = lax.axis_index("grp")
    core = lax.rem(g, 2)
    place = lax.div(g, 2)
    xl = lax.rem(place, 2)
    y = lax.div(place, 2)
    other_core = g + 1 - 2 * core
    other_x = g + 2 - 4 * xl
    ys = [lax.rem(y + k, 4) for k in range(4)]

    z = lax.rem(w, 8)
    xh = lax.div(w, 8)
    wides, even, odd = [], [], []
    for dx, dz in [(0, 4), (1, 4), (0, 3), (0, 5), (1, 3), (1, 5), (0, 2), (0, 6), (1, 2), (1, 6),
                   (0, 1), (0, 7), (1, 1), (1, 7), (1, 0)]:
        wides.append(lax.rem(xh + dx, 2) * 8 + lax.rem(z + dz, 8))
        (even, odd)[dz % 2].append(wides[-1])

    barrier = pltpu.get_barrier_semaphore()

    def greet(to_w, to_g):
        pl.semaphore_signal(barrier, inc=1, device_id=(to_w, to_g), device_id_type=MESH)

    for to in wides:
        greet(to, g)
    greet(w, other_core)
    greet(w, other_x)
    for k in (1, 3):
        greet(w, ys[k] * 4 + xl * 2 + core)

    into = (
        padded_rows.at[pl.ds(0, width)],
        padded_up.at[pl.ds(spare, width)],
        w_pair.at[pl.ds(0, width)],
        w_down.at[pl.ds(spare, width)],
    )
    copies = [
        pltpu.make_async_copy(src, dst, w_sem.at[i])
        for i, (src, dst) in enumerate(zip((rows_hbm, upstream_hbm, pair_hbm, down_hbm), into))
    ]
    for copy in copies:
        copy.start()
    padded_rows[pl.ds(width, spare), :] = jnp.zeros((spare, rows), BF16)
    padded_up[pl.ds(0, spare), :] = jnp.zeros((spare, rows), BF16)
    w_pair[pl.ds(width, spare), :] = jnp.zeros((spare, w_pair.shape[1]), BF16)
    w_down[pl.ds(0, spare), :] = jnp.zeros((spare, hidden), BF16)

    expert_row = route_ref[...]
    position = lax.broadcasted_iota(jnp.int32, (1, rows), 1)
    inside = position < live_ref[0]
    labels = lax.broadcasted_iota(jnp.int32, (experts, rows), 0)
    onehot = jnp.where((labels == expert_row) & inside, 1.0, 0.0).astype(F32)
    earlier = jnp.where(
        lax.broadcasted_iota(jnp.int32, (rows, rows), 0)
        < lax.broadcasted_iota(jnp.int32, (rows, rows), 1),
        1.0,
        0.0,
    ).astype(BF16)
    before = product(onehot.astype(BF16), earlier, 1, 0)
    rank = jnp.sum(before * onehot, axis=0, keepdims=True)
    counts = jnp.sum(onehot, axis=1, keepdims=True)
    count_out[...] = jnp.broadcast_to(counts, count_out.shape)
    expert_f = expert_row.astype(F32)
    probs_row = probs_ref[...]

    with jax.named_scope("load"):
        copies[0].wait()
        copies[1].wait()

    def remote(src, dst, send, recv, to_w, to_g):
        return pltpu.make_async_remote_copy(
            src_ref=src, dst_ref=dst, send_sem=send, recv_sem=recv,
            device_id=(to_w, to_g), device_id_type=MESH,
        )

    edge = packed - padded
    for c in range(chunks):
        slots = sizes[c]
        chunk_rows = experts * slots
        with jax.named_scope(f"arrange{c}"):
            offset = rank - float(firsts[c])
            fits = inside & (offset >= 0.0) & (offset < float(slots))
            target = jnp.where(fits, expert_f * float(slots) + offset, -1.0)
            index = lax.broadcasted_iota(jnp.int32, (chunk_rows, rows), 0).astype(F32)
            chosen = jnp.where(index == target, 1.0, 0.0).astype(F32)
            slot_prob = jnp.sum(chosen * probs_row, axis=1, keepdims=True)
            chosen = chosen.astype(BF16)
            select[c][...] = chosen
            row_part = product(chosen, padded_rows[...], 1, 1).astype(BF16)
            up_part = (slot_prob * product(chosen, padded_up[...], 1, 1)).astype(BF16)
            outgoing[c][:, :, pl.ds(0, edge)] = row_part[:, :edge].reshape(experts, slots, edge)
            outgoing[c][:, :, pl.ds(edge, padded - edge)] = (
                row_part[:, edge:] + up_part[:, : padded - edge]
            ).reshape(experts, slots, padded - edge)
            outgoing[c][:, :, pl.ds(padded, packed - padded)] = up_part[:, padded - edge :].reshape(
                experts, slots, packed - padded
            )
            incoming[c][lax.rem(w, 2), lax.div(w, 2)] = outgoing[c][w]
        if c == 0:
            with jax.named_scope("barrier"):
                pl.semaphore_wait(barrier, len(wides) + 4)
        with jax.named_scope(f"send{c}"):
            for to in wides:
                remote(
                    outgoing[c].at[to],
                    incoming[c].at[lax.rem(w, 2), lax.div(w, 2)],
                    disp_s.at[c], disp_r.at[c], to, g,
                ).start()
    count_in[w] = count_out[...]
    for to in wides:
        remote(count_out, count_in.at[w], count_s, count_r, to, g).start()

    with jax.named_scope("load2"):
        copies[2].wait()
        copies[3].wait()

    tile = 512

    def contract(c):
        slots = sizes[c]
        half_rows = both * slots
        await_bytes(outgoing[c].at[pl.ds(0, len(wides))], disp_r.at[c])

        def partial(parts, keep):
            def operand(first):
                blocks = [incoming[c][part, :, :, pl.ds(first, padded)] for part in parts]
                return jnp.concatenate(
                    [block.reshape(half_rows, padded) for block in blocks], axis=0
                )

            left, right = operand(0), operand(edge)

            @pl.loop(0, 2 * hidden // tile)
            def _(n):
                at = pl.ds(pl.multiple_of(n * tile, tile), tile)
                keep(at, product(left, w_pair[:, at], 1, 0))

            @pl.loop(0, hidden // tile)
            def _(n):
                at = pl.ds(pl.multiple_of(n * tile, tile), tile)
                to = pl.ds(pl.multiple_of(2 * hidden + n * tile, tile), tile)
                keep(to, product(right, w_down[:, at], 1, 0))

        def keep_out(at, value):
            core_out[c][:, :, at] = value[:half_rows].reshape(both, slots, tile).astype(BF16)

        def keep_own(at, value):
            own_sum[c][:, :, at] = value[-half_rows:].reshape(both, slots, tile)

        def keep_both(at, value):
            keep_out(at, value)
            keep_own(at, value)

        def exchange():
            remote(core_out[c], core_in[c], core_s.at[c], core_r.at[c], w, other_core).start()

        if half_rows < LANES:
            partial((1 - core, core), keep_both)
            exchange()
        else:
            partial((1 - core,), keep_out)
            exchange()
            partial((core,), keep_own)

    def to_y(k, src, dst, send, recv):
        remote(src, dst, send, recv, w, ys[k] * 4 + xl * 2 + core).start()

    def partial_sum(c, k, part):
        at = 2 * ys[k] + part
        return own_sum[c][at] + core_in[c][at].astype(F32)

    def reduce_y(c):
        await_bytes(core_in[c], core_r.at[c])
        for side in (0, 1):
            far_out[c][side] = partial_sum(c, 2, side).astype(BF16)
            to_y((1, 3)[side], far_out[c].at[side], far_in[c].at[side], far_s.at[c], far_r.at[c])
        for side in (0, 1):
            y_out[c][side, 1 - side] = partial_sum(c, (1, 3)[side], 1 - side).astype(BF16)
            to_y(
                (1, 3)[side], y_out[c].at[side, 1 - side], y_in[c].at[side, 1 - side],
                y_s.at[c], y_r.at[c],
            )

    def relay_y(c):
        await_bytes(far_in[c], far_r.at[c])
        for side in (0, 1):
            value = partial_sum(c, (1, 3)[side], side) + far_in[c][side].astype(F32)
            y_out[c][side, side] = value.astype(BF16)
            to_y(
                (1, 3)[side], y_out[c].at[side, side], y_in[c].at[side, side], y_s.at[c], y_r.at[c]
            )

    def reduce_x(c):
        await_bytes(y_in[c], y_r.at[c])

        def total(part):
            value = partial_sum(c, 0, part)
            for side in (0, 1):
                value = value + y_in[c][side, part].astype(F32)
            return value

        x_out[c][...] = total(1 - xl).astype(BF16)
        remote(x_out[c], x_in[c], x_s.at[c], x_r.at[c], w, other_x).start()
        x_own[c][...] = total(xl)

    def activate(c):
        slots = sizes[c]
        await_bytes(x_in[c], x_r.at[c])
        value = x_own[c][...] + x_in[c][...].astype(F32)
        gate = value[:, :hidden]
        up = value[:, hidden : 2 * hidden]
        grad_hidden = value[:, 2 * hidden :]
        sigmoid_gate = jax.nn.sigmoid(gate)
        swish = gate * sigmoid_gate
        act = (swish * up).astype(BF16)
        grad_gate = grad_hidden * up * sigmoid_gate * (1.0 + gate * (1.0 - sigmoid_gate))
        joined[c][core, place, :, pl.ds(0, hidden)] = act
        joined[c][core, place, :, pl.ds(hidden, hidden)] = grad_gate.astype(BF16)
        joined[c][core, place, :, pl.ds(2 * hidden, hidden)] = (grad_hidden * swish).astype(BF16)
        inner = jnp.sum(act.astype(F32) * grad_hidden, axis=1, keepdims=True)
        high = inner.astype(BF16).astype(F32)
        lane = lax.broadcasted_iota(jnp.int32, (slots, LANES), 1)
        at = width - (padded - LANES)
        split = jnp.where(lane == at, high, jnp.where(lane == at + 1, inner - high, 0.0))
        joined[c][core, place, :, pl.ds(3 * hidden, LANES)] = split.astype(BF16)
        for k in (1, 3):
            piece_to_y(c, k, place, gy_s, gy_r)
        remote(
            joined[c].at[core, place], joined[c].at[core, place], gx_s.at[c], gx_r.at[c], w, other_x
        ).start()

    def piece_to_y(c, k, at, send, recv):
        piece = joined[c].at[core, at]
        to_y(k, piece, piece, send.at[c], recv.at[c])

    cut_at = -(-joined[0].shape[3] // (2 * LANES)) * LANES

    def piece_to_x(c, at):
        piece = joined[c].at[core, at]
        remote(piece, piece, gx_s.at[c], gx_r.at[c], w, other_x).start()

    def half_to_y(c, k, at, first, size):
        piece = joined[c].at[core, at, :, pl.ds(first, size)]
        to_y(k, piece, piece, gf_s.at[c], gf_r.at[c])

    def forward(c):
        if c in COLUMN_FIRST:
            return
        await_bytes(joined[c].at[0, 0], gx_r.at[c])
        for k in (1, 3):
            piece_to_y(c, k, 2 * y + 1 - xl, gz_s, gz_r)

    def pass_near(c):
        await_bytes(joined[c].at[0, pl.ds(0, 2)], gy_r.at[c])
        if c in COLUMN_FIRST:
            half_to_y(c, 1, 2 * ys[3] + xl, 0, cut_at)
            half_to_y(c, 3, 2 * ys[1] + xl, cut_at, joined[0].shape[3] - cut_at)
            for k in (1, 3):
                piece_to_x(c, 2 * ys[k] + xl)
        else:
            piece_to_y(c, 1, 2 * ys[3] + xl, gf_s, gf_r)

    def pass_far(c):
        if c in COLUMN_FIRST:
            await_bytes(joined[c].at[0, 0], gf_r.at[c])
            piece_to_x(c, 2 * ys[2] + xl)
            for k in range(4):
                share(c, 2 * ys[k] + xl, 1)
            return
        await_bytes(joined[c].at[0, pl.ds(0, 2)], gz_r.at[c])
        piece_to_y(c, 3, 2 * ys[1] + 1 - xl, gf_s, gf_r)
        for k in (0, 1, 3):
            share(c, 2 * ys[k], 2)

    def share(c, at, count):
        pieces = joined[c].at[core, pl.ds(at, count)]
        remote(pieces, pieces, gc_s.at[c], gc_r.at[c], w, other_core).start()

    def share_last(c):
        if c in COLUMN_FIRST:
            await_bytes(joined[c].at[0, pl.ds(0, 4)], gx_r.at[c])
            for k in range(4):
                share(c, 2 * ys[k] + 1 - xl, 1)
            return
        await_bytes(joined[c].at[0, pl.ds(0, 2)], gf_r.at[c])
        share(c, 2 * ys[2], 2)

    def give_back(c):
        slots = sizes[c]
        half_rows = both * slots
        await_bytes(joined[c].at[0], gc_r.at[c])
        cut = padded - LANES

        def half(part, count):
            at = pl.ds(part, count)
            pairs = joined[c][at, :, :, pl.ds(hidden, 2 * hidden)]
            inner = joined[c][at, :, :, pl.ds(3 * hidden, LANES)]
            value = product(pairs.reshape(count * half_rows, 2 * hidden), w_pair[...], 1, 1)
            ret_out[c][at, :, :, pl.ds(0, cut)] = (
                value[:, :cut].astype(BF16).reshape(count, both, slots, cut)
            )
            ret_out[c][at, :, :, pl.ds(cut, LANES)] = (
                value[:, cut:].astype(BF16) + inner.reshape(count * half_rows, LANES)
            ).reshape(count, both, slots, LANES)

        def send(to):
            remote(
                ret_out[c].at[lax.rem(to, 2), lax.div(to, 2)], ret_in[c].at[w],
                ret_s.at[c], ret_r.at[c], to, g,
            ).start()

        if half_rows < LANES:
            half(0, 2)
            for to in wides:
                send(to)
        else:
            for number, group in enumerate((even, odd)):
                half(lax.rem(z + number, 2), 1)
                for to in group:
                    send(to)
        ret_in[c][w] = ret_out[c][lax.rem(w, 2), lax.div(w, 2)]

    def weigh():
        step = 256
        lefts, rights = [], []
        for c in range(chunks):
            chunk_rows = experts * sizes[c]
            lefts.append(incoming[c][:, :, :, pl.ds(0, padded)].reshape(chunk_rows, padded).T)
            rights.append(incoming[c][:, :, :, pl.ds(edge, padded)].reshape(chunk_rows, padded).T)

        def total(parts, at):
            value = 0.0
            for c in range(chunks):
                right = joined[c][:, :, :, at].reshape(experts * sizes[c], step)
                value = value + product(parts[c], right, 1, 0)
            return value

        @pl.loop(0, 2 * hidden // step)
        def _(n):
            at = pl.ds(pl.multiple_of(n * step, step), step)
            src = pl.ds(pl.multiple_of(hidden + n * step, step), step)
            pair_vm[:, at] = total(lefts, src)[:width].astype(BF16)

        @pl.loop(0, hidden // step)
        def _(n):
            at = pl.ds(pl.multiple_of(n * step, step), step)
            down_vm[:, at] = total(rights, at)[spare:].astype(BF16)

    def receive(c):
        chunk_rows = experts * sizes[c]
        await_bytes(outgoing[c].at[pl.ds(0, len(wides)), :, pl.ds(0, padded)], ret_r.at[c])
        value = product(ret_in[c][...].reshape(chunk_rows, padded), select[c][...], 0, 0)
        rows_acc[...] = value if c == 0 else rows_acc[...] + value

    order = (
        (contract, 0), (reduce_y, 0), (relay_y, 0), (reduce_x, 0), (contract, 1), (reduce_y, 1),
        (activate, 0), (relay_y, 1), (forward, 0), (pass_near, 0), (contract, 2), (reduce_y, 2),
        (reduce_x, 1), (pass_far, 0), (contract, 3), (reduce_y, 3), (relay_y, 2), (activate, 1),
        (relay_y, 3), (share_last, 0), (forward, 1), (reduce_x, 2), (give_back, 0),
        (pass_near, 1), (reduce_x, 3), (activate, 2), (pass_far, 1), (activate, 3), (forward, 2),
        (share_last, 1), (give_back, 1), (forward, 3), (pass_near, 2), (pass_near, 3),
        (pass_far, 2), (pass_far, 3), (share_last, 2), (share_last, 3), (give_back, 2),
        (give_back, 3),
    )
    for stage, c in order:
        with jax.named_scope(stage.__name__ + str(c)):
            stage(c)
    with jax.named_scope("weigh"):
        weigh()
    for c in range(chunks):
        with jax.named_scope(f"receive{c}"):
            receive(c)
    rows_vm[...] = rows_acc[pl.ds(0, width), :].astype(BF16)

    await_bytes(count_in.at[pl.ds(0, len(wides))], count_r)
    loads = jnp.sum(count_in[...], axis=0)[:, :1]
    share_row = jnp.sum(
        jnp.where(labels == expert_row, 1.0, 0.0) * (loads * (1.0 / rows)), axis=0, keepdims=True
    )
    inner = rows_acc[pl.ds(width, 8), :]
    inner_row = (inner[0:1] + inner[1:2]) / probs_row
    inner_row = inner_row.astype(BF16).astype(F32)
    grad_prob_ref[...] = jnp.where(inside, inner_row + BALANCE * share_row, 0.0)

    await_bytes(count_in.at[pl.ds(0, len(wides))], count_s)
    for c in range(chunks):
        await_bytes(outgoing[c].at[pl.ds(0, len(wides))], disp_s.at[c])
        await_bytes(core_out[c], core_s.at[c])
        await_bytes(far_out[c], far_s.at[c])
        await_bytes(y_out[c], y_s.at[c])
        await_bytes(x_out[c], x_s.at[c])
        await_bytes(joined[c].at[0, pl.ds(0, 2)], gy_s.at[c])
        if c in COLUMN_FIRST:
            await_bytes(joined[c].at[0, pl.ds(0, 4)], gx_s.at[c])
            await_bytes(joined[c].at[0, 0], gf_s.at[c])
        else:
            await_bytes(joined[c].at[0, 0], gx_s.at[c])
            await_bytes(joined[c].at[0, pl.ds(0, 2)], gz_s.at[c])
            await_bytes(joined[c].at[0, pl.ds(0, 2)], gf_s.at[c])
        await_bytes(joined[c].at[0], gc_s.at[c])
        await_bytes(outgoing[c].at[pl.ds(0, len(wides)), :, pl.ds(0, padded)], ret_s.at[c])


def store_kernel(rows_vm, prob_vm, pair_vm, down_vm, rows_hbm, prob_ref, pair_hbm, down_hbm, sem):
    copies = [
        pltpu.make_async_copy(src, dst, sem.at[i])
        for i, (src, dst) in enumerate(((pair_vm, pair_hbm), (down_vm, down_hbm), (rows_vm, rows_hbm)))
    ]
    for copy in copies:
        copy.start()
    prob_ref[...] = prob_vm[...].reshape(prob_ref.shape).astype(BF16)
    for copy in copies:
        copy.wait()


def on_device(rows_in, upstream, probs, route, live, gate_up, down):
    rows, width = rows_in.shape
    experts = lax.axis_size("wide")
    hidden = down.shape[1]
    unit = rows * 3 // (2 * experts) // sum(PARTS)
    sizes = [part * unit for part in PARTS]
    chunks = len(sizes)
    padded = -(-width // LANES) * LANES
    packed = 2 * width
    both = experts // 2
    total = 3 * hidden
    vmem = pltpu.VMEM
    dma = pltpu.SemaphoreType.DMA
    each = dma((chunks,))
    scratch = [
        vmem((padded, rows), BF16),
        vmem((padded, rows), BF16),
        [vmem((experts * slots, rows), BF16) for slots in sizes],
        [vmem((experts, slots, packed), BF16) for slots in sizes],
        [vmem((2, both, slots, packed), BF16) for slots in sizes],
        vmem((padded, 2 * hidden), BF16),
        vmem((padded, hidden), BF16),
        [vmem((both, slots, total), F32) for slots in sizes],
        [vmem((both, slots, total), BF16) for slots in sizes],
        [vmem((both, slots, total), BF16) for slots in sizes],
        [vmem((2, slots, total), BF16) for slots in sizes],
        [vmem((2, slots, total), BF16) for slots in sizes],
        [vmem((2, 2, slots, total), BF16) for slots in sizes],
        [vmem((2, 2, slots, total), BF16) for slots in sizes],
        [vmem((slots, total), F32) for slots in sizes],
        [vmem((slots, total), BF16) for slots in sizes],
        [vmem((slots, total), BF16) for slots in sizes],
        [vmem((2, both, slots, total + LANES), BF16) for slots in sizes],
        [vmem((2, both, slots, padded), BF16) for slots in sizes],
        [vmem((experts, slots, padded), BF16) for slots in sizes],
        vmem((padded, rows), F32),
        vmem((experts, LANES), F32),
        vmem((experts, experts, LANES), F32),
        dma((4,)),
        dma,
        dma,
    ] + [each] * 22
    in_vmem = pl.BlockSpec(memory_space=pltpu.VMEM)
    anywhere = pl.BlockSpec(memory_space=pltpu.HBM)
    out = pl.pallas_call(
        functools.partial(kernel, experts),
        out_shape=(
            vmem((width, rows), BF16),
            vmem((1, rows), F32),
            vmem((width, 2 * hidden), BF16),
            vmem((width, hidden), BF16),
        ),
        in_specs=[
            pl.BlockSpec(memory_space=pltpu.SMEM),
            anywhere,
            anywhere,
            in_vmem,
            in_vmem,
            anywhere,
            anywhere,
        ],
        out_specs=(in_vmem,) * 4,
        scratch_shapes=scratch,
        compiler_params=pltpu.CompilerParams(
            collective_id=0, has_side_effects=True, vmem_limit_bytes=121 * 2**19
        ),
    )(
        live,
        rows_in.T,
        upstream.T,
        probs.reshape(1, rows),
        route.reshape(1, rows),
        gate_up[0],
        down[0].T,
    )
    grad_rows, grad_prob, grad_pair, grad_down = pl.pallas_call(
        store_kernel,
        out_shape=(
            jax.ShapeDtypeStruct((width, rows), BF16),
            jax.ShapeDtypeStruct((rows,), BF16),
            jax.ShapeDtypeStruct((width, 2 * hidden), BF16),
            jax.ShapeDtypeStruct((width, hidden), BF16),
        ),
        in_specs=[in_vmem] * 4,
        out_specs=(anywhere, in_vmem, anywhere, anywhere),
        scratch_shapes=[dma((3,))],
        compiler_params=pltpu.CompilerParams(vmem_limit_bytes=2**20),
    )(*out)
    return (
        grad_rows.T,
        grad_prob,
        grad_pair[None],
        grad_down.T[None],
    )


def solution(mesh):
    return jax.shard_map(
        on_device,
        mesh=mesh,
        in_specs=(
            P("wide", "grp"),
            P("wide", "grp"),
            P("wide"),
            P("wide", None),
            P("wide"),
            P("wide", "grp", None),
            P("wide", None, "grp"),
        ),
        out_specs=(P("wide", "grp"), P("wide"), P("wide", "grp", None), P("wide", None, "grp")),
        check_vma=False,
    )
```
